32 devices in a mesh: gx: 4 (over y, x), gy: 8 (over z, core).
Axes of the slice: x: 2, y: 2, z: 4, core: 2. Of those that a mesh axis runs over, the one named last changes fastest.
Arguments:
- right_side: float32 [256, 256, 256], P('gx', 'gy'), may hold values from -45 to 45
- block_inverse: float32 [1, 256, 256], replicated, may hold values from -1 to 2
- basis_left: float32 [2, 1, 32, 256], replicated, may hold values from -0.25 to 0.25
- basis_right: float32 [2, 1, 32, 256], replicated, may hold values from -0.25 to 0.25
- ranks: int32 [2, 1, 256, 256], replicated, may hold values from 1 to 32
Outputs:
- solution_field: float32 [256, 256, 256], P('gx', 'gy')
- true_gap: float32 [256, 256, 256], P('gx', 'gy')
- preconditioned: float32 [256, 256, 256], P('gx', 'gy')
The draws below stay inside these ranges and needn't reach their ends.
All inputs are finite; a program needn't handle non-finite values.
Results may differ from the reference program's by a relative error of at most 0.0003.
Values sent between devices are 32-bit elements; how exact they have to be, the bound alone decides.
No kernel may reach another device: no remote copies, remote signals or barrier semaphores. Data moves between devices by JAX's collectives and lax.ppermute only.
A program may use at most 64 MiB of HBM per device.

```python
import math
import jax
import jax.numpy as jnp
from jax import lax

NZ = 256
BLOCK = 256
RANK = 32
ITERS = 2
NZB = 1
NX = 256
NY = 256


def draw_right_side(key, part):
    first = jax.random.fold_in(jax.random.fold_in(key, 11), 0)
    along_x = (jnp.arange(NX, dtype=jnp.float32) / NX)[:, None, None]
    along_y = (jnp.arange(NY, dtype=jnp.float32) / NY)[None, :, None]
    scales = 3.0 ** along_x * 3.0 ** along_y
    rough = jax.random.truncated_normal(first, -5.0, 5.0, (NX, NY, NZ), jnp.float32)
    return rough * scales


def draw_block_inverse(key, part):
    inner = jax.random.fold_in(key, 23)
    sigma = 0.2 / math.sqrt(BLOCK)
    noise = jax.random.normal(inner, (NZB, BLOCK, BLOCK), jnp.float32)
    symmetric = (noise + jnp.swapaxes(noise, 1, 2)) * (sigma / math.sqrt(2.0))
    return jnp.eye(BLOCK, dtype=jnp.float32)[None, :, :] + symmetric


def with_ends(entries, rng, least, largest):
    longest = entries.shape.index(max(entries.shape))
    spots = []
    for shift in (0, 1):
        where = [jax.random.randint(jax.random.fold_in(rng, axis), (), 0, length) for axis, length in enumerate(entries.shape)]
        where[longest] = (where[longest] + shift) % entries.shape[longest]
        spots.append(tuple(where))
    return entries.at[spots[0]].set(least).at[spots[1]].set(largest)


def gaussian(rng, shape, scale, reach, kind=jnp.bfloat16):
    return jnp.clip(scale * jax.random.normal(rng, shape, jnp.float32), -reach, reach).astype(kind)


def setup_inputs(seed: int = 0) -> dict:
    arg_keys = jax.random.split(jax.random.key(seed), 6)
    right_side = draw_right_side(jax.random.fold_in(arg_keys[5], 71), 0)
    block_inverse = draw_block_inverse(jax.random.fold_in(arg_keys[5], 71), 0)
    basis_left = gaussian(arg_keys[2], (2, NZB, RANK, BLOCK), (0.3 / BLOCK ** 0.5), 0.25, jnp.float32)
    basis_right = gaussian(arg_keys[3], (2, NZB, RANK, BLOCK), (0.3 / BLOCK ** 0.5), 0.25, jnp.float32)
    ranks = with_ends(jax.random.randint(arg_keys[4], (2, NZB, NX, NY), 1, RANK + 1), jax.random.fold_in(arg_keys[4], 1), 1, RANK).astype(jnp.int32)
    return dict(right_side=right_side, block_inverse=block_inverse, basis_left=basis_left, basis_right=basis_right, ranks=ranks)


mass_shift = 0.05


def operate(field):
    beside = jnp.roll(field, 1, 0) + jnp.roll(field, -1, 0)
    beside = beside + jnp.roll(field, 1, 1) + jnp.roll(field, -1, 1)
    beside = beside + jnp.roll(field, 1, 2) + jnp.roll(field, -1, 2)
    return (6.0 + mass_shift) * field - beside


def couple_term(source, factor_in, factor_out, limits, levels):
    coef = jnp.einsum('xybc,bkc->xybk', source, factor_in, precision=lax.Precision.HIGHEST)
    keep = levels[None, None, None, :] < jnp.transpose(limits, (1, 2, 0))[..., None]
    coef = jnp.where(keep, coef, jnp.zeros_like(coef))
    return jnp.einsum('xybk,bki->xybi', coef, factor_out, precision=lax.Precision.HIGHEST)


def precondition(residual, block_inverse, basis_left, basis_right, ranks):
    nx, ny, nz = residual.shape
    nzb = block_inverse.shape[0]
    blk = block_inverse.shape[1]
    rank = basis_left.shape[2]
    blocks = residual.reshape(nx, ny, nzb, blk)
    total = jnp.einsum('xybc,bic->xybi', blocks, block_inverse, precision=lax.Precision.HIGHEST)
    levels = jnp.arange(rank, dtype=jnp.int32)
    for along in range(2):
        ahead = jnp.roll(blocks, -1, along)
        total = total + couple_term(ahead, basis_right[along], basis_left[along], ranks[along], levels)
        behind = jnp.roll(blocks, 1, along)
        limits = jnp.roll(ranks[along], 1, along + 1)
        total = total + couple_term(behind, basis_left[along], basis_right[along], limits, levels)
    return total.reshape(nx, ny, nz)


def reference(right_side, block_inverse, basis_left, basis_right, ranks):
    solution_field = jnp.zeros_like(right_side)
    residual = right_side
    precond = precondition(residual, block_inverse, basis_left, basis_right, ranks)
    direction = precond
    rz_now = jnp.sum(residual * precond)
    for step in range(ITERS):
        image = operate(direction)
        alpha = rz_now / jnp.sum(direction * image)
        solution_field = solution_field + alpha * direction
        residual = residual - alpha * image
        precond = precondition(residual, block_inverse, basis_left, basis_right, ranks)
        if step + 1 < ITERS:
            rz_next = jnp.sum(residual * precond)
            direction = precond + (rz_next / rz_now) * direction
            rz_now = rz_next
    true_gap = right_side - operate(solution_field)
    return solution_field, true_gap, precond
```

```python
import jax
import jax.numpy as jnp
from jax import lax
from jax.experimental import pallas as pl
from jax.experimental.pallas import tpu as pltpu
from jax.sharding import PartitionSpec as P

F32 = jnp.float32
BF16 = jnp.bfloat16
DIAGONAL = 6.0 + 0.05
DEPTH = 5
PAD = 8
NT = (((1,), (1,)), ((), ()))
NN = (((1,), (0,)), ((), ()))
TN = (((0,), (0,)), ((), ()))
WHOLE = pl.BlockSpec(memory_space=pltpu.VMEM)
GRANT = pltpu.CompilerParams(vmem_limit_bytes=16 << 20)


def largest_divisor(count, limit):
    return max(d for d in range(1, limit + 1) if count % d == 0)


def dot(left, right, dims):
    return lax.dot_general(left, right, dims, preferred_element_type=F32)


def halves(value):
    high = value.astype(BF16)
    low = (value - high.astype(F32)).astype(BF16)
    return high, low


def inward(inverse, left, right):
    square = halves(inverse[0])
    factors = jnp.concatenate([right[0, 0], left[0, 0], right[1, 0], left[1, 0]], 0)
    narrow = halves(factors)
    return square, (jnp.concatenate(narrow, 0), narrow[0])


def outward(left, right):
    factors = jnp.concatenate([left[0, 0], right[0, 0], left[1, 0], right[1, 0]], 0)
    high, low = halves(factors)
    return jnp.concatenate([high, high], 0), low


def diagonal_part(high, low, square):
    return dot(high, square[0], NT) + dot(high, square[1], NT) + dot(low, square[0], NT)


def coefficients(high, low, narrow):
    both = dot(high, narrow[0], NT)
    rank = both.shape[1] // 2
    return both[:, :rank] + both[:, rank:] + dot(low, narrow[1], NT)


def coupling_part(coefs, factors):
    high, low = halves(coefs)
    return dot(jnp.concatenate([high, low], 1), factors[0], NN) + dot(high, factors[1], NN)


def gathered(coef_ref, start, rows, stride, limit):
    here = coef_ref[pl.ds(start, rows)]
    lane = lax.broadcasted_iota(jnp.int32, here.shape, 1)
    quarter = here.shape[1] // 4
    ahead_x = coef_ref[pl.ds(pl.multiple_of(start + stride, 8), rows)]
    behind_x = coef_ref[pl.ds(pl.multiple_of(start - stride, 8), rows)]
    ahead_y = pltpu.roll(here, rows - 1, 0)
    behind_y = pltpu.roll(here, 1, 0)
    along_x = jnp.where(lane < quarter, ahead_x, behind_x)
    along_y = jnp.where(lane < 3 * quarter, ahead_y, behind_y)
    picked = jnp.where(lane < 2 * quarter, along_x, along_y)
    level = lax.rem(lane, quarter).astype(F32)
    return jnp.where(level < limit, picked, 0.0)


def operated(ref, start, rows, stride):
    here = ref[pl.ds(start, rows)]
    width = here.shape[1]
    beside = ref[pl.ds(pl.multiple_of(start + stride, 8), rows)]
    beside = beside + ref[pl.ds(pl.multiple_of(start - stride, 8), rows)]
    beside = beside + pltpu.roll(here, rows - 1, 0) + pltpu.roll(here, 1, 0)
    beside = beside + pltpu.roll(here, width - 1, 1) + pltpu.roll(here, 1, 1)
    return DIAGONAL * here - beside


def own_kernel(stride, block, inverse, left, right, diag_out, coef_out):
    cells_x, cells_y, width = block.shape
    square, narrow = inward(inverse, left, right)
    step = largest_divisor(cells_x, 8)

    def body(i, carry):
        rows = block[pl.ds(i * step, step)].reshape(step * cells_y, width)
        high, low = halves(rows)
        diag = diagonal_part(high, low, square)
        coef = coefficients(high, low, narrow)
        for j in range(step):
            at = pl.multiple_of((i * step + j + DEPTH) * stride + PAD, 8)
            diag_out[pl.ds(at, cells_y)] = diag[j * cells_y : (j + 1) * cells_y]
            coef_out[pl.ds(at, cells_y)] = coef[j * cells_y : (j + 1) * cells_y]
        return carry

    lax.fori_loop(0, cells_x // step, body, 0)


def side_kernel(stride, diag_in, coef_in, low_x, high_x, low_y, high_y, inverse, left, right, diag_out, coef_out, turned):
    square, narrow = inward(inverse, left, right)
    depth, cells_y, width = low_x.shape
    cells_x = low_y.shape[1]
    for ref, first in ((low_x, 0), (high_x, DEPTH + cells_x)):
        high, low = halves(ref[...].reshape(depth * cells_y, width))
        diag = diagonal_part(high, low, square)
        coef = coefficients(high, low, narrow)
        for j in range(depth):
            at = (first + j) * stride + PAD
            diag_out[pl.ds(at, cells_y)] = diag[j * cells_y : (j + 1) * cells_y]
            coef_out[pl.ds(at, cells_y)] = coef[j * cells_y : (j + 1) * cells_y]
    for ref, inside, edge in ((low_y, PAD - DEPTH, 0), (high_y, 0, PAD + cells_y)):
        high, low = halves(ref[...].reshape(depth * cells_x, width))
        diag = diagonal_part(high, low, square)
        coef = coefficients(high, low, narrow)
        for j in range(depth):
            part = slice(j * cells_x, (j + 1) * cells_x)
            at = pl.ds(inside + j, cells_x, stride=PAD)
            for k in range(width // 128):
                turned[k, at] = diag[part, k * 128 : (k + 1) * 128]
            turned[width // 128, at] = coef[part]

        def place(x, carry):
            here = pl.ds(pl.multiple_of(x * PAD, 8), PAD)
            at = pl.ds(pl.multiple_of((x + DEPTH) * stride + edge, 8), PAD)
            for k in range(width // 128):
                diag_out[at, pl.ds(k * 128, 128)] = turned[k, here]
            coef_out[at] = turned[width // 128, here]
            return carry

        lax.fori_loop(0, cells_x, place, 0, unroll=4)


def chain_kernel(
    stride, diag_in, coef_in, low_x, high_x, limits, block, inverse, left, right,
    first, coef, first_image, second, second_image, limit, sums,
):
    cells_x, cells_y, width = block.shape
    square, narrow = inward(inverse, left, right)
    factors = outward(left, right)
    near = DEPTH - 1

    for ref, edge, sign in ((low_x, DEPTH - near, -1), (high_x, DEPTH + cells_x, 1)):
        count = ref.shape[0] * ref.shape[1]
        high, low = halves(ref[...].reshape(count, width))
        diag = diagonal_part(high, low, square)
        coefs = coefficients(high, low, narrow)
        for j in range(2 * near):
            away_y = near - j if j < near else j - near + 1
            y = PAD - away_y if j < near else PAD + cells_y + away_y - 1
            for i in range(near):
                away_x = near - i if sign < 0 else i + 1
                if away_x + away_y <= DEPTH:
                    at = (edge + i) * stride + y
                    row = j * near + i
                    first[pl.ds(at, 1)] = diag[row : row + 1]
                    coef[pl.ds(at, 1)] = coefs[row : row + 1]

    kinds = limits.shape[0]
    lane = lax.broadcasted_iota(jnp.int32, (kinds, coef.shape[1]), 1)
    kind = lax.broadcasted_iota(jnp.int32, (kinds, coef.shape[1]), 0)
    spread = jnp.where(lane // (coef.shape[1] // 4) == kind, 1.0, 0.0).astype(BF16)

    def spread_limits(i, carry):
        at = pl.multiple_of(i * 128, 128)
        limit[pl.ds(at, 128)] = dot(limits[:, pl.ds(at, 128)], spread, TN)
        return carry

    lax.fori_loop(0, limits.shape[1] // 128, spread_limits, 0)

    def slabs(begin, end, most, work):
        step = largest_divisor(end - begin, most)

        def body(i, carry):
            return work(pl.multiple_of((begin + i * step) * stride, 8), step * stride, carry)

        return body, (end - begin) // step

    def couple(ref):
        def work(start, rows, carry):
            at = pl.ds(start, rows)
            picked = gathered(coef, start, rows, stride, limit[at])
            ref[at] = ref[at] + coupling_part(picked, factors)
            return carry

        return work

    def image_and_project(start, rows, carry):
        at = pl.ds(start, rows)
        image = operated(first, start, rows, stride)
        first_image[at] = image
        high, low = halves(image)
        second[at] = diagonal_part(high, low, square)
        coef[at] = coefficients(high, low, narrow)
        return carry

    def last_image(start, rows, carry):
        second_image[pl.ds(start, rows)] = operated(second, start, rows, stride)
        return carry

    last = 2 * DEPTH + cells_x
    body, count = slabs(1, last - 1, 9, couple(first))
    lax.fori_loop(0, count, body, 0)
    body, count = slabs(2, last - 2, 9, image_and_project)
    lax.fori_loop(0, count, body, 0)
    body, count = slabs(3, last - 3, 9, couple(second))
    lax.fori_loop(0, count, body, 0)
    body, count = slabs(4, last - 4, 9, last_image)
    lax.fori_loop(0, count, body, 0)

    def fold(value):
        return jnp.sum(value.reshape(cells_y // 8, 8, width), 0)

    def products(x, carry):
        at = pl.ds(pl.multiple_of((x + DEPTH) * stride + PAD, 8), cells_y)
        rhs = block[x]
        z0, w0, u0, v0 = first[at], first_image[at], second[at], second_image[at]
        terms = (rhs * z0, z0 * w0, rhs * u0, w0 * u0, u0 * v0)
        return tuple(c + fold(t) for c, t in zip(carry, terms))

    zero = jnp.zeros((8, width), F32)
    parts = lax.fori_loop(0, cells_x, products, (zero,) * 5)
    rows = [jnp.sum(jnp.sum(p, 0, keepdims=True), 1, keepdims=True) for p in parts]
    for i, row in enumerate(rows):
        sums[pl.ds(i, 1)] = jnp.broadcast_to(row, (1, sums.shape[1]))
    sums[pl.ds(5, 3)] = jnp.zeros((3, sums.shape[1]), F32)


def last_kernel(stride, begin, field, limit, inverse, left, right, out, coef):
    step, cells_y, width = out.shape
    square, narrow = inward(inverse, left, right)
    factors = outward(left, right)
    start = (begin + DEPTH) * stride
    high, low = halves(field[pl.ds(start - stride, (step + 2) * stride)])
    coef[...] = coefficients(high, low, narrow)
    picked = gathered(coef, stride, step * stride, stride, limit[pl.ds(start, step * stride)])
    picked = picked.reshape(step, stride, picked.shape[1])[:, PAD : PAD + cells_y]
    rows = field[pl.ds(start, step * stride)].reshape(step, stride, width)[:, PAD : PAD + cells_y]
    high, low = halves(rows.reshape(step * cells_y, width))
    total = diagonal_part(high, low, square)
    total = total + coupling_part(picked.reshape(step * cells_y, picked.shape[2]), factors)
    out[...] = total.reshape(step, cells_y, width)


def combine_kernel(stride, step, pieces, sums, block, z_ref, w_ref, u_ref, v_ref, *rest):
    y_refs, (solution_out, gap_out, precond_out) = rest[:pieces], rest[pieces:]
    i = pl.program_id(0)
    cells_y = block.shape[1]
    rz, zw, ru, wu, uv = (sums[pl.ds(k, 1), pl.ds(0, 128)] for k in range(5))
    alpha = rz / zw
    rz_next = alpha * (alpha * wu - ru)
    ratio = rz_next / rz
    grown = 1.0 + ratio
    curve = grown * (grown * zw - 2.0 * alpha * wu) + alpha * alpha * uv
    alpha_next = rz_next / curve
    s = jnp.concatenate([alpha + alpha_next * grown] * (block.shape[2] // 128), 1)
    t = jnp.concatenate([alpha * alpha_next] * (block.shape[2] // 128), 1)

    def work(y_ref):
        for j in range(step):
            x = i * step + j
            at = pl.ds(pl.multiple_of((x + DEPTH) * stride + PAD, 8), cells_y)
            z0, w0, u0, v0 = z_ref[at], w_ref[at], u_ref[at], v_ref[at]
            solution_out[j] = s * z0 - t * u0
            gap_out[j] = (block[j] - s * w0) + t * v0
            precond_out[j] = (z0 - s * u0) + t * y_ref[lax.rem(x, y_ref.shape[0])]

    per = y_refs[0].shape[0] // step
    for k in range(pieces):
        pl.when(lax.div(i, per) == k)(lambda k=k: work(y_refs[k]))


def resident(*values):
    return tuple(pltpu.with_memory_space_constraint(v, pltpu.VMEM) for v in values)


def neighbour(value, axis, offset):
    count = lax.axis_size(axis)
    return lax.ppermute(value, axis, [(i, (i + offset) % count) for i in range(count)])


def wrapped(table, axis, begin, size, before, after):
    length = table.shape[axis]
    head = lax.slice_in_dim(table, length - before, length, axis=axis)
    tail = lax.slice_in_dim(table, 0, after, axis=axis)
    whole = jnp.concatenate([head, table, tail], axis)
    return lax.dynamic_slice_in_dim(whole, begin, size + before + after, axis)


def total_over(value, axis):
    count = lax.axis_size(axis)
    if count & (count - 1):
        return lax.psum(value, axis)
    hop = 1
    while hop < count:
        value = value + lax.ppermute(value, axis, [(i, i ^ hop) for i in range(count)])
        hop *= 2
    return value


def per_device(right_side, block_inverse, basis_left, basis_right, ranks):
    cells_x, cells_y, width = right_side.shape
    stride = cells_y + 2 * PAD
    lines = (cells_x + 2 * DEPTH) * stride
    padded = -(-lines // 128) * 128
    rank4 = 4 * basis_left.shape[2]
    weights = (block_inverse, basis_left, basis_right)
    wide = pltpu.VMEM((lines, width), F32)
    slim = pltpu.VMEM((lines, rank4), F32)

    low_y = neighbour(jnp.transpose(right_side[:, cells_y - DEPTH :], (1, 0, 2)), "gy", 1)
    high_y = neighbour(jnp.transpose(right_side[:, :DEPTH], (1, 0, 2)), "gy", -1)
    low_x = neighbour(right_side[cells_x - DEPTH :], "gx", 1)
    high_x = neighbour(right_side[:DEPTH], "gx", -1)

    diag, coef = pl.pallas_call(
        lambda *refs: own_kernel(stride, *refs),
        out_shape=(wide, slim), in_specs=[WHOLE] * 4, out_specs=(WHOLE,) * 2, name="own", compiler_params=GRANT,
    )(*resident(right_side, *weights))

    table = wrapped(ranks[:, 0], 1, lax.axis_index("gx") * cells_x, cells_x, DEPTH + 1, DEPTH)
    table = wrapped(table, 2, lax.axis_index("gy") * cells_y, cells_y, PAD + 1, PAD)
    limits = jnp.stack([table[0, 1:, 1:], table[0, :-1, 1:], table[1, 1:, 1:], table[1, 1:, :-1]])
    limits = jnp.pad(limits.reshape(4, lines).astype(F32), ((0, 4), (0, padded - lines))).astype(BF16)

    near = DEPTH - 1
    corners = jnp.concatenate([low_y[1:], high_y[:near]], 0)
    corner_low = neighbour(corners[:, cells_x - near :], "gx", 1)
    corner_high = neighbour(corners[:, :near], "gx", -1)

    diag, coef = pl.pallas_call(
        lambda *refs: side_kernel(stride, *refs),
        out_shape=(wide, slim), in_specs=[WHOLE] * 9, out_specs=(WHOLE,) * 2,
        input_output_aliases={0: 0, 1: 1}, name="side", compiler_params=GRANT,
        scratch_shapes=[pltpu.VMEM((width // 128 + 1, cells_x * PAD, 128), F32)],
    )(*resident(diag, coef, low_x, high_x, low_y, high_y, *weights))

    first, _, first_image, second, second_image, limit, sums = pl.pallas_call(
        lambda *refs: chain_kernel(stride, *refs),
        out_shape=(
            wide, slim, wide, wide, wide,
            pltpu.VMEM((padded, rank4), F32), pltpu.VMEM((8, 128), F32),
        ),
        in_specs=[WHOLE] * 9, out_specs=(WHOLE,) * 7,
        input_output_aliases={0: 0, 1: 1}, name="chain", compiler_params=GRANT,
    )(*resident(diag, coef, corner_low, corner_high, limits, right_side, *weights))

    sums = total_over(total_over(sums, "gx"), "gy")

    pieces = 4 if cells_x % 4 == 0 else 1
    step = cells_x // pieces
    last = [
        pl.pallas_call(
            lambda *refs, k=k: last_kernel(stride, k * step, *refs),
            out_shape=pltpu.VMEM((step, cells_y, width), F32),
            in_specs=[WHOLE] * 5, out_specs=WHOLE,
            scratch_shapes=[pltpu.VMEM(((step + 2) * stride, rank4), F32)], name="last", compiler_params=GRANT,
        )(*resident(second_image, limit, *weights))
        for k in range(pieces)
    ]

    chunk = largest_divisor(step, 8)
    tile = pl.BlockSpec((chunk, cells_y, width), lambda i: (i, 0, 0))
    out = jax.ShapeDtypeStruct((cells_x, cells_y, width), F32)
    return pl.pallas_call(
        lambda *refs: combine_kernel(stride, chunk, pieces, *refs),
        grid=(cells_x // chunk,),
        out_shape=(out,) * 3,
        in_specs=[WHOLE, tile] + [WHOLE] * (4 + pieces), out_specs=(tile,) * 3, name="combine", compiler_params=GRANT,
    )(*resident(sums), right_side, *resident(first, first_image, second, second_image, *last))


def solution(mesh):
    placed = (P("gx", "gy", None), P(), P(), P(), P())
    return jax.shard_map(
        per_device,
        mesh=mesh,
        in_specs=placed,
        out_specs=(P("gx", "gy", None), P("gx", "gy", None), P("gx", "gy", None)),
        check_vma=False,
    )
```

```python
import jax
import jax.numpy as jnp
from jax import lax
from jax.experimental import pallas as pl
from jax.experimental.pallas import tpu as pltpu
from jax.sharding import PartitionSpec as P


F32 = jnp.float32
BF16 = jnp.bfloat16
DIAGONAL = 6.0 + 0.05
DEPTH = 5
PAD = 8
NT = (((1,), (1,)), ((), ()))
NN = (((1,), (0,)), ((), ()))
WHOLE = pl.BlockSpec(memory_space=pltpu.VMEM)
GRANT = pltpu.CompilerParams(vmem_limit_bytes=16 << 20)


def largest_divisor(count, limit):
    return max(d for d in range(1, limit + 1) if count % d == 0)


def dot(left, right, dims):
    return lax.dot_general(left, right, dims, preferred_element_type=F32)


def halves(value):
    high = value.astype(BF16)
    low = (value - high.astype(F32)).astype(BF16)
    return high, low


def inward(inverse, left, right):
    square = halves(inverse[0])
    factors = jnp.concatenate([right[0, 0], left[0, 0], right[1, 0], left[1, 0]], 0)
    narrow = halves(factors)
    return square, (jnp.concatenate(narrow, 0), narrow[0])


def outward(left, right):
    factors = jnp.concatenate([left[0, 0], right[0, 0], left[1, 0], right[1, 0]], 0)
    high, low = halves(factors)
    return jnp.concatenate([high, high], 0), low


def diagonal_part(high, low, square):
    return dot(high, square[0], NT) + dot(high, square[1], NT) + dot(low, square[0], NT)


def coefficients(high, low, narrow):
    both = dot(high, narrow[0], NT)
    rank = both.shape[1] // 2
    return both[:, :rank] + both[:, rank:] + dot(low, narrow[1], NT)


def coupling_part(coefs, factors):
    high, low = halves(coefs)
    return dot(jnp.concatenate([high, low], 1), factors[0], NN) + dot(high, factors[1], NN)


def gathered(coef_ref, start, rows, stride, limit):
    here = coef_ref[pl.ds(start, rows)]
    lane = lax.broadcasted_iota(jnp.int32, here.shape, 1)
    quarter = here.shape[1] // 4
    ahead_x = coef_ref[pl.ds(pl.multiple_of(start + stride, 8), rows)]
    behind_x = coef_ref[pl.ds(pl.multiple_of(start - stride, 8), rows)]
    ahead_y = pltpu.roll(here, rows - 1, 0)
    behind_y = pltpu.roll(here, 1, 0)
    along_x = jnp.where(lane < quarter, ahead_x, behind_x)
    along_y = jnp.where(lane < 3 * quarter, ahead_y, behind_y)
    picked = jnp.where(lane < 2 * quarter, along_x, along_y)
    level = lax.rem(lane, quarter)
    return jnp.where(level < limit, picked, 0.0)


def operated(ref, start, rows, stride):
    here = ref[pl.ds(start, rows)]
    width = here.shape[1]
    beside = ref[pl.ds(pl.multiple_of(start + stride, 8), rows)]
    beside = beside + ref[pl.ds(pl.multiple_of(start - stride, 8), rows)]
    beside = beside + pltpu.roll(here, rows - 1, 0) + pltpu.roll(here, 1, 0)
    beside = beside + pltpu.roll(here, width - 1, 1) + pltpu.roll(here, 1, 1)
    return DIAGONAL * here - beside


def pack_kernel(source, block, low_x, high_x, low_y, high_y, arrived):
    cells_x, cells_y, _ = block.shape
    step = cells_x // arrived.shape[0]
    parts = [pl.ds(i * step, step) for i in range(arrived.shape[0])]
    copies = [pltpu.make_async_copy(source.at[p], block.at[p], arrived.at[i]) for i, p in enumerate(parts)]
    for copy in copies:
        copy.start()
    for copy, part in zip(copies, parts):
        copy.wait()
        for j in range(DEPTH):
            low_y[j, part] = block[part, j]
            high_y[j, part] = block[part, cells_y - DEPTH + j]
    low_x[...] = block[pl.ds(0, DEPTH)]
    high_x[...] = block[pl.ds(cells_x - DEPTH, DEPTH)]


def corner_kernel(low_y, high_y, low_x, high_x):
    near = DEPTH - 1
    cells_x = low_y.shape[1]
    for ref, first in ((low_x, 0), (high_x, cells_x - near)):
        at = pl.ds(first, near)
        ref[pl.ds(0, near)] = low_y[pl.ds(1, near), at]
        ref[pl.ds(near, near)] = high_y[pl.ds(0, near), at]


def table_kernel(stride, cells_x, cells_y, ranks, limit, rows, arrived):
    length_x, length_y = ranks.shape[2], ranks.shape[3]
    begin = lax.axis_index("gx") * cells_x
    parts = (
        (lax.rem(begin - PAD + length_x, length_x), 0, PAD),
        (begin, PAD, cells_x),
        (lax.rem(begin + cells_x, length_x), PAD + cells_x, PAD),
    )
    copies = [
        pltpu.make_async_copy(
            ranks.at[e, 0, pl.ds(pl.multiple_of(source, 8), size)],
            rows.at[e, pl.ds(target, size)],
            arrived.at[e, k],
        )
        for e in range(2)
        for k, (source, target, size) in enumerate(parts)
    ]
    for copy in copies:
        copy.start()
    for copy in copies:
        copy.wait()
    turn = lax.rem(PAD + length_y - lax.axis_index("gy") * cells_y, length_y)
    tall = rows.shape[1]
    here = [pltpu.roll(pltpu.roll(rows[e], turn, 1), tall - PAD + DEPTH, 0) for e in range(2)]
    kinds = (here[0], pltpu.roll(here[0], 1, 0), here[1], pltpu.roll(here[1], 1, 1))
    shape = (tall, limit.shape[1])
    kind = lax.broadcasted_iota(jnp.int32, shape, 1) // (shape[1] // 4)
    for y in range(PAD - DEPTH + 1, PAD + cells_y + DEPTH - 1):
        column = [jnp.broadcast_to(k[:, y : y + 1], shape) for k in kinds]
        along_x = jnp.where(kind == 0, column[0], column[1])
        along_y = jnp.where(kind == 2, column[2], column[3])
        limit[pl.ds(y, tall, stride=stride)] = jnp.where(kind < 2, along_x, along_y)


def own_kernel(stride, block, inverse, left, right, diag_out, coef_out):
    cells_x, cells_y, width = block.shape
    square, narrow = inward(inverse, left, right)
    step = largest_divisor(cells_x, 8)

    def body(i, carry):
        rows = block[pl.ds(i * step, step)].reshape(step * cells_y, width)
        high, low = halves(rows)
        diag = diagonal_part(high, low, square)
        coef = coefficients(high, low, narrow)
        for j in range(step):
            at = pl.multiple_of((i * step + j + DEPTH) * stride + PAD, 8)
            diag_out[pl.ds(at, cells_y)] = diag[j * cells_y : (j + 1) * cells_y]
            coef_out[pl.ds(at, cells_y)] = coef[j * cells_y : (j + 1) * cells_y]
        return carry

    lax.fori_loop(0, cells_x // step, body, 0)


def side_kernel(stride, diag_in, coef_in, low_x, high_x, low_y, high_y, inverse, left, right, diag_out, coef_out, turned):
    square, narrow = inward(inverse, left, right)
    depth, cells_y, width = low_x.shape
    cells_x = low_y.shape[1]
    for ref, first in ((low_x, 0), (high_x, DEPTH + cells_x)):
        high, low = halves(ref[...].reshape(depth * cells_y, width))
        diag = diagonal_part(high, low, square)
        coef = coefficients(high, low, narrow)
        for j in range(depth):
            at = (first + j) * stride + PAD
            diag_out[pl.ds(at, cells_y)] = diag[j * cells_y : (j + 1) * cells_y]
            coef_out[pl.ds(at, cells_y)] = coef[j * cells_y : (j + 1) * cells_y]
    for ref, inside, edge in ((low_y, PAD - DEPTH, 0), (high_y, 0, PAD + cells_y)):
        high, low = halves(ref[...].reshape(depth * cells_x, width))
        diag = diagonal_part(high, low, square)
        coef = coefficients(high, low, narrow)
        for j in range(depth):
            part = slice(j * cells_x, (j + 1) * cells_x)
            at = pl.ds(inside + j, cells_x, stride=PAD)
            for k in range(width // 128):
                turned[k, at] = diag[part, k * 128 : (k + 1) * 128]
            turned[width // 128, at] = coef[part]

        def place(x, carry):
            here = pl.ds(pl.multiple_of(x * PAD, 8), PAD)
            at = pl.ds(pl.multiple_of((x + DEPTH) * stride + edge, 8), PAD)
            for k in range(width // 128):
                diag_out[at, pl.ds(k * 128, 128)] = turned[k, here]
            coef_out[at] = turned[width // 128, here]
            return carry

        lax.fori_loop(0, cells_x, place, 0, unroll=4)


def chain_kernel(
    stride, diag_in, coef_in, low_x, high_x, limit, block, inverse, left, right,
    first, coef, first_image, second, second_image, sums,
):
    cells_x, cells_y, width = block.shape
    square, narrow = inward(inverse, left, right)
    factors = outward(left, right)
    near = DEPTH - 1

    for ref, edge, sign in ((low_x, DEPTH - near, -1), (high_x, DEPTH + cells_x, 1)):
        count = ref.shape[0] * ref.shape[1]
        high, low = halves(ref[...].reshape(count, width))
        diag = diagonal_part(high, low, square)
        coefs = coefficients(high, low, narrow)
        for j in range(2 * near):
            away_y = near - j if j < near else j - near + 1
            y = PAD - away_y if j < near else PAD + cells_y + away_y - 1
            for i in range(near):
                away_x = near - i if sign < 0 else i + 1
                if away_x + away_y <= DEPTH:
                    at = (edge + i) * stride + y
                    row = j * near + i
                    first[pl.ds(at, 1)] = diag[row : row + 1]
                    coef[pl.ds(at, 1)] = coefs[row : row + 1]

    def slabs(begin, end, most, work):
        step = largest_divisor(end - begin, most)

        def body(i, carry):
            return work(pl.multiple_of((begin + i * step) * stride, 8), step * stride, carry)

        return body, (end - begin) // step

    def couple(ref):
        def work(start, rows, carry):
            at = pl.ds(start, rows)
            picked = gathered(coef, start, rows, stride, limit[at])
            ref[at] = ref[at] + coupling_part(picked, factors)
            return carry

        return work

    def image_and_project(start, rows, carry):
        at = pl.ds(start, rows)
        image = operated(first, start, rows, stride)
        first_image[at] = image
        high, low = halves(image)
        second[at] = diagonal_part(high, low, square)
        coef[at] = coefficients(high, low, narrow)
        return carry

    def last_image(start, rows, carry):
        second_image[pl.ds(start, rows)] = operated(second, start, rows, stride)
        return carry

    last = 2 * DEPTH + cells_x
    body, count = slabs(1, last - 1, 9, couple(first))
    lax.fori_loop(0, count, body, 0, unroll=True)
    body, count = slabs(2, last - 2, 9, image_and_project)
    lax.fori_loop(0, count, body, 0, unroll=True)
    body, count = slabs(3, last - 3, 9, couple(second))
    lax.fori_loop(0, count, body, 0, unroll=True)
    body, count = slabs(4, last - 4, 9, last_image)
    lax.fori_loop(0, count, body, 0, unroll=True)

    def fold(value):
        return jnp.sum(value.reshape(cells_y // 8, 8, width), 0)

    def products(x, carry):
        at = pl.ds(pl.multiple_of((x + DEPTH) * stride + PAD, 8), cells_y)
        rhs = block[x]
        z0, w0, u0, v0 = first[at], first_image[at], second[at], second_image[at]
        terms = (rhs * z0, z0 * w0, rhs * u0, w0 * u0, u0 * v0)
        return tuple(c + fold(t) for c, t in zip(carry, terms))

    zero = jnp.zeros((8, width), F32)
    parts = lax.fori_loop(0, cells_x, products, (zero,) * 5)
    rows = [jnp.sum(jnp.sum(p, 0, keepdims=True), 1, keepdims=True) for p in parts]
    for i, row in enumerate(rows):
        sums[pl.ds(i, 1)] = jnp.broadcast_to(row, (1, sums.shape[1]))
    sums[pl.ds(5, 3)] = jnp.zeros((3, sums.shape[1]), F32)


def last_kernel(stride, begin, field, limit, inverse, left, right, out, coef):
    step, cells_y, width = out.shape
    square, narrow = inward(inverse, left, right)
    factors = outward(left, right)
    start = (begin + DEPTH) * stride
    high, low = halves(field[pl.ds(start - stride, (step + 2) * stride)])
    coef[...] = coefficients(high, low, narrow)
    picked = gathered(coef, stride, step * stride, stride, limit[pl.ds(start, step * stride)])
    picked = picked.reshape(step, stride, picked.shape[1])[:, PAD : PAD + cells_y]
    rows = field[pl.ds(start, step * stride)].reshape(step, stride, width)[:, PAD : PAD + cells_y]
    high, low = halves(rows.reshape(step * cells_y, width))
    total = diagonal_part(high, low, square)
    total = total + coupling_part(picked.reshape(step * cells_y, picked.shape[2]), factors)
    out[...] = total.reshape(step, cells_y, width)


def combine_kernel(stride, step, pieces, sums, block, z_ref, w_ref, u_ref, v_ref, *rest):
    y_refs, outs, buffers, sent = rest[:pieces], rest[pieces : pieces + 3], rest[pieces + 3 : pieces + 6], rest[-1]
    cells_x, cells_y, width = block.shape
    rz, zw, ru, wu, uv = (sums[pl.ds(k, 1), pl.ds(0, 128)] for k in range(5))
    alpha = rz / zw
    rz_next = alpha * (alpha * wu - ru)
    ratio = rz_next / rz
    grown = 1.0 + ratio
    curve = grown * (grown * zw - 2.0 * alpha * wu) + alpha * alpha * uv
    alpha_next = rz_next / curve
    s = jnp.concatenate([alpha + alpha_next * grown] * (width // 128), 1)
    t = jnp.concatenate([alpha * alpha_next] * (width // 128), 1)

    def copies(chunk):
        part = pl.ds(chunk * step, step)
        return [
            pltpu.make_async_copy(buffer.at[part], out.at[part], sent.at[k, chunk])
            for k, (buffer, out) in enumerate(zip(buffers, outs))
        ]

    per = cells_x // pieces // step

    def work(i, carry, k):
        chunk = k * per + i
        for j in range(step):
            x = chunk * step + j
            at = pl.ds(pl.multiple_of((x + DEPTH) * stride + PAD, 8), cells_y)
            z0, w0, u0, v0 = z_ref[at], w_ref[at], u_ref[at], v_ref[at]
            buffers[0][x] = s * z0 - t * u0
            buffers[1][x] = (block[x] - s * w0) + t * v0
            buffers[2][x] = (z0 - s * u0) + t * y_refs[k][i * step + j]
        for copy in copies(chunk):
            copy.start()
        return carry

    for k in range(pieces):
        lax.fori_loop(0, per, lambda i, carry, k=k: work(i, carry, k), 0)

    def finish(chunk, carry):
        for copy in copies(chunk):
            copy.wait()
        return carry

    lax.fori_loop(0, cells_x // step, finish, 0)


def resident(*values):
    return tuple(pltpu.with_memory_space_constraint(v, pltpu.VMEM) for v in values)


def neighbour(value, axis, offset):
    count = lax.axis_size(axis)
    return lax.ppermute(value, axis, [(i, (i + offset) % count) for i in range(count)])


def total_over(value, axis):
    count = lax.axis_size(axis)
    if count & (count - 1):
        return lax.psum(value, axis)
    hop = 1
    while hop < count:
        moved = lax.ppermute(value, axis, [(i, i ^ hop) for i in range(count)])
        value = value + moved
        hop *= 2
    return value


def call(kernel, out_shape, inputs, specs=None, **kwargs):
    return pl.pallas_call(
        kernel, out_shape=out_shape, in_specs=specs or [WHOLE] * len(inputs), compiler_params=GRANT, **kwargs
    )(*inputs)


def per_device(right_side, block_inverse, basis_left, basis_right, ranks):
    cells_x, cells_y, width = right_side.shape
    stride = cells_y + 2 * PAD
    lines = (cells_x + 2 * DEPTH) * stride
    tall = cells_x + 2 * PAD
    rank4 = 4 * basis_left.shape[2]
    near = DEPTH - 1
    weights = resident(block_inverse, basis_left, basis_right)
    wide = pltpu.VMEM((lines, width), F32)
    slim = pltpu.VMEM((lines, rank4), F32)
    edge_x = pltpu.VMEM((DEPTH, cells_y, width), F32)
    edge_y = pltpu.VMEM((DEPTH, cells_x, width), F32)
    corner = pltpu.VMEM((2 * near, near, width), F32)

    anywhere = pl.BlockSpec(memory_space=pltpu.HBM)
    block, out_x, in_x, out_y, in_y = call(
        pack_kernel, (pltpu.VMEM(right_side.shape, F32), edge_x, edge_x, edge_y, edge_y), (pltpu.with_memory_space_constraint(right_side, pltpu.HBM),),
        [anywhere], out_specs=(WHOLE,) * 5,
        scratch_shapes=[pltpu.SemaphoreType.DMA((cells_x // largest_divisor(cells_x, 8),))],
    )
    (block,) = resident(block)
    low_y = neighbour(in_y, "gy", 1)
    high_y = neighbour(out_y, "gy", -1)
    low_x = neighbour(in_x, "gx", 1)
    high_x = neighbour(out_x, "gx", -1)

    diag, coef = call(lambda *refs: own_kernel(stride, *refs), (wide, slim), (block, *weights), out_specs=(WHOLE,) * 2)
    limit = call(
        lambda *refs: table_kernel(stride, cells_x, cells_y, *refs),
        pltpu.VMEM((tall * stride, rank4), jnp.int32), (ranks,), [pl.BlockSpec(memory_space=pl.ANY)],
        out_specs=WHOLE,
        scratch_shapes=[pltpu.VMEM((2, tall, ranks.shape[3]), jnp.int32), pltpu.SemaphoreType.DMA((2, 3))],
    )

    corners = call(corner_kernel, (corner, corner), resident(low_y, high_y), out_specs=(WHOLE,) * 2)
    corner_low = neighbour(corners[1], "gx", 1)
    corner_high = neighbour(corners[0], "gx", -1)

    diag, coef = call(
        lambda *refs: side_kernel(stride, *refs), (wide, slim),
        (*resident(diag, coef, low_x, high_x, low_y, high_y), *weights), out_specs=(WHOLE,) * 2,
        input_output_aliases={0: 0, 1: 1},
        scratch_shapes=[pltpu.VMEM((width // 128 + 1, cells_x * PAD, 128), F32)],
    )

    first, _, first_image, second, second_image, sums = call(
        lambda *refs: chain_kernel(stride, *refs),
        (wide, slim, wide, wide, wide, pltpu.VMEM((8, 128), F32)),
        (*resident(diag, coef, corner_low, corner_high, limit), block, *weights), out_specs=(WHOLE,) * 6,
        input_output_aliases={0: 0, 1: 1},
    )

    sums = total_over(total_over(sums, "gx"), "gy")

    pieces = 4 if cells_x % 4 == 0 else 1
    step = cells_x // pieces
    last = [
        call(
            lambda *refs, k=k: last_kernel(stride, k * step, *refs),
            pltpu.VMEM((step, cells_y, width), F32), (*resident(second_image, limit), *weights), out_specs=WHOLE,
            scratch_shapes=[pltpu.VMEM(((step + 2) * stride, rank4), F32)],
        )
        for k in range(pieces)
    ]

    chunk = largest_divisor(step, 4)
    out = jax.ShapeDtypeStruct((cells_x, cells_y, width), F32)
    return call(
        lambda *refs: combine_kernel(stride, chunk, pieces, *refs), (out,) * 3,
        (*resident(sums), block, *resident(first, first_image, second, second_image, *last)),
        out_specs=(anywhere,) * 3,
        scratch_shapes=[pltpu.VMEM((cells_x, cells_y, width), F32)] * 3
        + [pltpu.SemaphoreType.DMA((3, cells_x // chunk))],
    )


def solution(mesh):
    placed = (P("gx", "gy", None), P(), P(), P(), P())

    return jax.shard_map(
        per_device,
        mesh=mesh,
        in_specs=placed,
        out_specs=(P("gx", "gy", None), P("gx", "gy", None), P("gx", "gy", None)),
        check_vma=False,
    )
```

```python
import jax
import jax.numpy as jnp
from jax import lax
from jax.experimental import pallas as pl
from jax.experimental.pallas import tpu as pltpu
from jax.sharding import PartitionSpec as P


F32 = jnp.float32
BF16 = jnp.bfloat16
DIAGONAL = 6.0 + 0.05
DEPTH = 5
PAD = 8
NT = (((1,), (1,)), ((), ()))
NN = (((1,), (0,)), ((), ()))
WHOLE = pl.BlockSpec(memory_space=pltpu.VMEM)
GRANT = pltpu.CompilerParams(vmem_limit_bytes=16 << 20)


def largest_divisor(count, limit):
    return max(d for d in range(1, limit + 1) if count % d == 0)


def dot(left, right, dims):
    return lax.dot_general(left, right, dims, preferred_element_type=F32)


def halves(value):
    high = value.astype(BF16)
    low = (value - high.astype(F32)).astype(BF16)
    return high, low


def inward(inverse, left, right):
    square = halves(inverse[0])
    factors = jnp.concatenate([right[0, 0], left[0, 0], right[1, 0], left[1, 0]], 0)
    narrow = halves(factors)
    return square, (jnp.concatenate(narrow, 0), narrow[0])


def outward(left, right):
    factors = jnp.concatenate([left[0, 0], right[0, 0], left[1, 0], right[1, 0]], 0)
    high, low = halves(factors)
    return jnp.concatenate([high, high], 0), low


def diagonal_part(high, low, square):
    return dot(high, square[0], NT) + dot(high, square[1], NT) + dot(low, square[0], NT)


def coefficients(high, low, narrow):
    both = dot(high, narrow[0], NT)
    rank = both.shape[1] // 2
    return both[:, :rank] + both[:, rank:] + dot(low, narrow[1], NT)


def coupling_part(coefs, factors):
    high, low = halves(coefs)
    return dot(jnp.concatenate([high, low], 1), factors[0], NN) + dot(high, factors[1], NN)


def gathered(coef_ref, start, rows, stride, limit):
    here = coef_ref[pl.ds(start, rows)]
    lane = lax.broadcasted_iota(jnp.int32, here.shape, 1)
    quarter = here.shape[1] // 4
    ahead_x = coef_ref[pl.ds(pl.multiple_of(start + stride, 8), rows)]
    behind_x = coef_ref[pl.ds(pl.multiple_of(start - stride, 8), rows)]
    ahead_y = pltpu.roll(here, rows - 1, 0)
    behind_y = pltpu.roll(here, 1, 0)
    along_x = jnp.where(lane < quarter, ahead_x, behind_x)
    along_y = jnp.where(lane < 3 * quarter, ahead_y, behind_y)
    picked = jnp.where(lane < 2 * quarter, along_x, along_y)
    level = lax.rem(lane, quarter)
    return jnp.where(level < limit, picked, 0.0)


def operated(ref, start, rows, stride):
    here = ref[pl.ds(start, rows)]
    width = here.shape[1]
    beside = ref[pl.ds(pl.multiple_of(start + stride, 8), rows)]
    beside = beside + ref[pl.ds(pl.multiple_of(start - stride, 8), rows)]
    beside = beside + pltpu.roll(here, rows - 1, 0) + pltpu.roll(here, 1, 0)
    beside = beside + pltpu.roll(here, width - 1, 1) + pltpu.roll(here, 1, 1)
    return DIAGONAL * here - beside


def pack_kernel(source, block, low_x, high_x, low_y, high_y, arrived):
    cells_x, cells_y, _ = block.shape
    step = cells_x // arrived.shape[0]
    parts = [pl.ds(i * step, step) for i in range(arrived.shape[0])]
    copies = [pltpu.make_async_copy(source.at[p], block.at[p], arrived.at[i]) for i, p in enumerate(parts)]
    for copy in copies:
        copy.start()
    for copy, part in zip(copies, parts):
        copy.wait()
        for j in range(DEPTH):
            low_y[j, part] = block[part, j]
            high_y[j, part] = block[part, cells_y - DEPTH + j]
    low_x[...] = block[pl.ds(0, DEPTH)]
    high_x[...] = block[pl.ds(cells_x - DEPTH, DEPTH)]


def corner_kernel(low_y, high_y, low_x, high_x):
    near = DEPTH - 1
    cells_x = low_y.shape[1]
    for ref, first in ((low_x, 0), (high_x, cells_x - near)):
        at = pl.ds(first, near)
        ref[pl.ds(0, near)] = low_y[pl.ds(1, near), at]
        ref[pl.ds(near, near)] = high_y[pl.ds(0, near), at]


def table_kernel(stride, cells_x, cells_y, ranks, limit, rows, arrived):
    length_x, length_y = ranks.shape[2], ranks.shape[3]
    begin = lax.axis_index("gx") * cells_x
    parts = (
        (lax.rem(begin - PAD + length_x, length_x), 0, PAD),
        (begin, PAD, cells_x),
        (lax.rem(begin + cells_x, length_x), PAD + cells_x, PAD),
    )
    copies = [
        pltpu.make_async_copy(
            ranks.at[e, 0, pl.ds(pl.multiple_of(source, 8), size)],
            rows.at[e, pl.ds(target, size)],
            arrived.at[e, k],
        )
        for e in range(2)
        for k, (source, target, size) in enumerate(parts)
    ]
    for copy in copies:
        copy.start()
    for copy in copies:
        copy.wait()
    turn = lax.rem(PAD + length_y - lax.axis_index("gy") * cells_y, length_y)
    tall = rows.shape[1]
    here = [pltpu.roll(pltpu.roll(rows[e], turn, 1), tall - PAD + DEPTH, 0) for e in range(2)]
    kinds = (here[0], pltpu.roll(here[0], 1, 0), here[1], pltpu.roll(here[1], 1, 1))
    shape = (tall, limit.shape[1])
    kind = lax.broadcasted_iota(jnp.int32, shape, 1) // (shape[1] // 4)
    for y in range(PAD - DEPTH + 1, PAD + cells_y + DEPTH - 1):
        column = [jnp.broadcast_to(k[:, y : y + 1], shape) for k in kinds]
        along_x = jnp.where(kind == 0, column[0], column[1])
        along_y = jnp.where(kind == 2, column[2], column[3])
        limit[pl.ds(y, tall, stride=stride)] = jnp.where(kind < 2, along_x, along_y)


def own_kernel(stride, block, inverse, left, right, diag_out, coef_out):
    cells_x, cells_y, width = block.shape
    square, narrow = inward(inverse, left, right)
    step = largest_divisor(cells_x, 8)

    def body(i, carry):
        rows = block[pl.ds(i * step, step)].reshape(step * cells_y, width)
        high, low = halves(rows)
        diag = diagonal_part(high, low, square)
        coef = coefficients(high, low, narrow)
        for j in range(step):
            at = pl.multiple_of((i * step + j + DEPTH) * stride + PAD, 8)
            diag_out[pl.ds(at, cells_y)] = diag[j * cells_y : (j + 1) * cells_y]
            coef_out[pl.ds(at, cells_y)] = coef[j * cells_y : (j + 1) * cells_y]
        return carry

    lax.fori_loop(0, cells_x // step, body, 0, unroll=True)


def side_kernel(stride, diag_in, coef_in, low_x, high_x, low_y, high_y, inverse, left, right, diag_out, coef_out, turned):
    square, narrow = inward(inverse, left, right)
    depth, cells_y, width = low_x.shape
    cells_x = low_y.shape[1]
    for ref, first in ((low_x, 0), (high_x, DEPTH + cells_x)):
        high, low = halves(ref[...].reshape(depth * cells_y, width))
        diag = diagonal_part(high, low, square)
        coef = coefficients(high, low, narrow)
        for j in range(depth):
            at = (first + j) * stride + PAD
            diag_out[pl.ds(at, cells_y)] = diag[j * cells_y : (j + 1) * cells_y]
            coef_out[pl.ds(at, cells_y)] = coef[j * cells_y : (j + 1) * cells_y]
    for ref, inside, edge in ((low_y, PAD - DEPTH, 0), (high_y, 0, PAD + cells_y)):
        high, low = halves(ref[...].reshape(depth * cells_x, width))
        diag = diagonal_part(high, low, square)
        coef = coefficients(high, low, narrow)
        for j in range(depth):
            part = slice(j * cells_x, (j + 1) * cells_x)
            at = pl.ds(inside + j, cells_x, stride=PAD)
            for k in range(width // 128):
                turned[k, at] = diag[part, k * 128 : (k + 1) * 128]
            turned[width // 128, at] = coef[part]

        def place(x, carry):
            here = pl.ds(pl.multiple_of(x * PAD, 8), PAD)
            at = pl.ds(pl.multiple_of((x + DEPTH) * stride + edge, 8), PAD)
            for k in range(width // 128):
                diag_out[at, pl.ds(k * 128, 128)] = turned[k, here]
            coef_out[at] = turned[width // 128, here]
            return carry

        lax.fori_loop(0, cells_x, place, 0, unroll=4)


def chain_kernel(
    stride, diag_in, coef_in, low_x, high_x, limit, block, inverse, left, right,
    first, coef, first_image, second, sums,
):
    cells_x, cells_y, width = block.shape
    square, narrow = inward(inverse, left, right)
    factors = outward(left, right)
    near = DEPTH - 1

    for ref, edge, sign in ((low_x, DEPTH - near, -1), (high_x, DEPTH + cells_x, 1)):
        count = ref.shape[0] * ref.shape[1]
        high, low = halves(ref[...].reshape(count, width))
        diag = diagonal_part(high, low, square)
        coefs = coefficients(high, low, narrow)
        for j in range(2 * near):
            away_y = near - j if j < near else j - near + 1
            y = PAD - away_y if j < near else PAD + cells_y + away_y - 1
            for i in range(near):
                away_x = near - i if sign < 0 else i + 1
                if away_x + away_y <= DEPTH:
                    at = (edge + i) * stride + y
                    row = j * near + i
                    first[pl.ds(at, 1)] = diag[row : row + 1]
                    coef[pl.ds(at, 1)] = coefs[row : row + 1]

    def slabs(begin, end, most):
        step = largest_divisor(end - begin, most)
        return [(x, step) for x in range(begin, end, step)]

    def inside(value, x, step):
        value = value.reshape(step, stride, value.shape[1])[:, PAD : PAD + cells_y]
        return value[max(DEPTH - x, 0) : max(DEPTH + cells_x - x, 0)]

    def owned(x, step):
        return max(x - DEPTH, 0), min(x + step - DEPTH, cells_x)

    def summed(value):
        return jnp.sum(value.reshape(-1, 8, width), 0)

    totals = [jnp.zeros((8, width), F32)] * 6
    last = 2 * DEPTH + cells_x
    for x, step in slabs(1, last - 1, 9):
        at = pl.ds(x * stride, step * stride)
        picked = gathered(coef, x * stride, step * stride, stride, limit[at])
        first[at] = first[at] + coupling_part(picked, factors)
    for x, step in slabs(2, last - 2, 9):
        at = pl.ds(x * stride, step * stride)
        image = operated(first, x * stride, step * stride, stride)
        first_image[at] = image
        high, low = halves(image)
        second[at] = diagonal_part(high, low, square)
        coef[at] = coefficients(high, low, narrow)
        begin, end = owned(x, step)
        if begin < end:
            field = inside(first[at], x, step)
            totals[0] += summed(block[pl.ds(begin, end - begin)] * field)
            totals[1] += summed(inside(image, x, step) * field)
    for x, step in slabs(3, last - 3, 9):
        at = pl.ds(x * stride, step * stride)
        picked = gathered(coef, x * stride, step * stride, stride, limit[at])
        field = second[at] + coupling_part(picked, factors)
        second[at] = field
        begin, end = owned(x, step)
        if begin < end:
            field = inside(field, x, step)
            totals[2] += summed(block[pl.ds(begin, end - begin)] * field)
            totals[3] += summed(inside(first_image[at], x, step) * field)
            totals[4] += summed(field * field)
    for x, step in slabs(DEPTH, DEPTH + cells_x, 8):
        start, rows = x * stride, step * stride
        here = second[pl.ds(start, rows)]
        beside = second[pl.ds(start + stride, rows)] + pltpu.roll(here, rows - 1, 0) + pltpu.roll(here, width - 1, 1)
        totals[5] += summed(inside(here * beside, x, step))
    totals = totals[:4] + [DIAGONAL * totals[4] - 2.0 * totals[5]]
    rows = [jnp.sum(jnp.sum(p, 0, keepdims=True), 1, keepdims=True) for p in totals]
    for i, row in enumerate(rows):
        sums[pl.ds(i, 1)] = jnp.broadcast_to(row, (1, sums.shape[1]))
    sums[pl.ds(5, 3)] = jnp.zeros((3, sums.shape[1]), F32)


def last_kernel(stride, begin, field, limit, inverse, left, right, image_out, out, image, coef):
    step, cells_y, width = out.shape
    square, narrow = inward(inverse, left, right)
    factors = outward(left, right)
    start = (begin + DEPTH) * stride
    part = largest_divisor(step + 2, 9)
    for x in range(0, step + 2, part):
        at = pl.ds(x * stride, part * stride)
        value = operated(field, start + (x - 1) * stride, part * stride, stride)
        image[at] = value
        coef[at] = coefficients(*halves(value), narrow)
    picked = gathered(coef, stride, step * stride, stride, limit[pl.ds(start, step * stride)])
    picked = picked.reshape(step, stride, picked.shape[1])[:, PAD : PAD + cells_y]
    rows = image[pl.ds(stride, step * stride)].reshape(step, stride, width)[:, PAD : PAD + cells_y]
    image_out[...] = rows
    high, low = halves(rows.reshape(step * cells_y, width))
    total = diagonal_part(high, low, square)
    total = total + coupling_part(picked.reshape(step * cells_y, picked.shape[2]), factors)
    out[...] = total.reshape(step, cells_y, width)


def combine_kernel(stride, step, pieces, sums, block, z_ref, w_ref, u_ref, *rest):
    v_refs, y_refs, rest = rest[0 : 2 * pieces : 2], rest[1 : 2 * pieces : 2], rest[2 * pieces :]
    outs, buffers, sent = rest[:3], rest[3:6], rest[6]
    cells_x, cells_y, width = block.shape
    rz, zw, ru, wu, uv = (sums[pl.ds(k, 1), pl.ds(0, 128)] for k in range(5))
    alpha = rz / zw
    rz_next = alpha * (alpha * wu - ru)
    ratio = rz_next / rz
    grown = 1.0 + ratio
    curve = grown * (grown * zw - 2.0 * alpha * wu) + alpha * alpha * uv
    alpha_next = rz_next / curve
    s = jnp.concatenate([alpha + alpha_next * grown] * (width // 128), 1)
    t = jnp.concatenate([alpha * alpha_next] * (width // 128), 1)

    def copies(chunk):
        part = pl.ds(chunk * step, step)
        return [
            pltpu.make_async_copy(buffer.at[part], out.at[part], sent.at[k, chunk])
            for k, (buffer, out) in enumerate(zip(buffers, outs))
        ]

    per = cells_x // pieces // step

    def work(i, carry, k):
        chunk = k * per + i
        for j in range(step):
            x = chunk * step + j
            at = pl.ds(pl.multiple_of((x + DEPTH) * stride + PAD, 8), cells_y)
            z0, w0, u0 = z_ref[at], w_ref[at], u_ref[at]
            buffers[0][x] = s * z0 - t * u0
            buffers[1][x] = (block[x] - s * w0) + t * v_refs[k][i * step + j]
            buffers[2][x] = (z0 - s * u0) + t * y_refs[k][i * step + j]
        for copy in copies(chunk):
            copy.start()
        return carry

    for k in range(pieces):
        lax.fori_loop(0, per, lambda i, carry, k=k: work(i, carry, k), 0, unroll=True)

    def finish(chunk, carry):
        for copy in copies(chunk):
            copy.wait()
        return carry

    lax.fori_loop(0, cells_x // step, finish, 0)


def resident(*values):
    return tuple(pltpu.with_memory_space_constraint(v, pltpu.VMEM) for v in values)


def neighbour(value, axis, offset):
    count = lax.axis_size(axis)
    return lax.ppermute(value, axis, [(i, (i + offset) % count) for i in range(count)])


def total_over(value, axis):
    count = lax.axis_size(axis)
    if count & (count - 1):
        return lax.psum(value, axis)
    hop = 1
    while hop < count:
        moved = lax.ppermute(value, axis, [(i, i ^ hop) for i in range(count)])
        value = value + moved
        hop *= 2
    return value


def call(kernel, out_shape, inputs, specs=None, **kwargs):
    return pl.pallas_call(
        kernel, out_shape=out_shape, in_specs=specs or [WHOLE] * len(inputs), compiler_params=GRANT, **kwargs
    )(*inputs)


def per_device(right_side, block_inverse, basis_left, basis_right, ranks):
    cells_x, cells_y, width = right_side.shape
    stride = cells_y + 2 * PAD
    lines = (cells_x + 2 * DEPTH) * stride
    tall = cells_x + 2 * PAD
    rank4 = 4 * basis_left.shape[2]
    near = DEPTH - 1
    weights = resident(block_inverse, basis_left, basis_right)
    wide = pltpu.VMEM((lines, width), F32)
    slim = pltpu.VMEM((lines, rank4), F32)
    edge_x = pltpu.VMEM((DEPTH, cells_y, width), F32)
    edge_y = pltpu.VMEM((DEPTH, cells_x, width), F32)
    corner = pltpu.VMEM((2 * near, near, width), F32)

    anywhere = pl.BlockSpec(memory_space=pltpu.HBM)
    block, out_x, in_x, out_y, in_y = call(
        pack_kernel, (pltpu.VMEM(right_side.shape, F32), edge_x, edge_x, edge_y, edge_y), (pltpu.with_memory_space_constraint(right_side, pltpu.HBM),),
        [anywhere], out_specs=(WHOLE,) * 5,
        scratch_shapes=[pltpu.SemaphoreType.DMA((cells_x // largest_divisor(cells_x, 8),))],
    )
    (block,) = resident(block)
    low_y = neighbour(in_y, "gy", 1)
    high_y = neighbour(out_y, "gy", -1)
    low_x = neighbour(in_x, "gx", 1)
    high_x = neighbour(out_x, "gx", -1)

    diag, coef = call(lambda *refs: own_kernel(stride, *refs), (wide, slim), (block, *weights), out_specs=(WHOLE,) * 2)
    limit = call(
        lambda *refs: table_kernel(stride, cells_x, cells_y, *refs),
        pltpu.VMEM((tall * stride, rank4), jnp.int32), (ranks,), [pl.BlockSpec(memory_space=pl.ANY)],
        out_specs=WHOLE,
        scratch_shapes=[pltpu.VMEM((2, tall, ranks.shape[3]), jnp.int32), pltpu.SemaphoreType.DMA((2, 3))],
    )

    corners = call(corner_kernel, (corner, corner), resident(low_y, high_y), out_specs=(WHOLE,) * 2)
    corner_low = neighbour(corners[1], "gx", 1)
    corner_high = neighbour(corners[0], "gx", -1)

    diag, coef = call(
        lambda *refs: side_kernel(stride, *refs), (wide, slim),
        (*resident(diag, coef, low_x, high_x, low_y, high_y), *weights), out_specs=(WHOLE,) * 2,
        input_output_aliases={0: 0, 1: 1},
        scratch_shapes=[pltpu.VMEM((width // 128 + 1, cells_x * PAD, 128), F32)],
    )

    first, _, first_image, second, sums = call(
        lambda *refs: chain_kernel(stride, *refs),
        (wide, slim, wide, wide, pltpu.VMEM((8, 128), F32)),
        (*resident(diag, coef, corner_low, corner_high, limit), block, *weights), out_specs=(WHOLE,) * 5,
        input_output_aliases={0: 0, 1: 1},
    )

    sums = total_over(total_over(sums, "gx"), "gy")

    pieces = 4 if cells_x % 4 == 0 else 1
    step = cells_x // pieces
    piece = pltpu.VMEM((step, cells_y, width), F32)
    last = [
        array
        for k in range(pieces)
        for array in call(
            lambda *refs, k=k: last_kernel(stride, k * step, *refs), (piece, piece),
            (*resident(second, limit), *weights), out_specs=(WHOLE,) * 2,
            scratch_shapes=[pltpu.VMEM(((step + 2) * stride, n), F32) for n in (width, rank4)],
        )
    ]

    chunk = largest_divisor(step, 8)
    out = jax.ShapeDtypeStruct((cells_x, cells_y, width), F32)
    return call(
        lambda *refs: combine_kernel(stride, chunk, pieces, *refs), (out,) * 3,
        (*resident(sums), block, *resident(first, first_image, second, *last)),
        out_specs=(anywhere,) * 3,
        scratch_shapes=[pltpu.VMEM((cells_x, cells_y, width), F32)] * 3
        + [pltpu.SemaphoreType.DMA((3, cells_x // chunk))],
    )


def solution(mesh):
    placed = (P("gx", "gy", None), P(), P(), P(), P())

    return jax.shard_map(
        per_device,
        mesh=mesh,
        in_specs=placed,
        out_specs=(P("gx", "gy", None), P("gx", "gy", None), P("gx", "gy", None)),
        check_vma=False,
    )
```

```python
import jax
import jax.numpy as jnp
from jax import lax
from jax.experimental import pallas as pl
from jax.experimental.pallas import tpu as pltpu
from jax.sharding import PartitionSpec as P


F32 = jnp.float32
BF16 = jnp.bfloat16
DIAGONAL = 6.0 + 0.05
DEPTH = 5
PAD = 8
NT = (((1,), (1,)), ((), ()))
NN = (((1,), (0,)), ((), ()))
WHOLE = pl.BlockSpec(memory_space=pltpu.VMEM)
GRANT = pltpu.CompilerParams(vmem_limit_bytes=16 << 20)


def largest_divisor(count, limit):
    return max(d for d in range(1, limit + 1) if count % d == 0)


def dot(left, right, dims):
    return lax.dot_general(left, right, dims, preferred_element_type=F32)


def halves(value):
    high = value.astype(BF16)
    low = (value - high.astype(F32)).astype(BF16)
    return high, low


def inward(inverse, left, right):
    square = halves(inverse[0])
    factors = jnp.concatenate([right[0, 0], left[0, 0], right[1, 0], left[1, 0]], 0)
    narrow = halves(factors)
    return square, (jnp.concatenate(narrow, 0), narrow[0])


def outward(left, right):
    factors = jnp.concatenate([left[0, 0], right[0, 0], left[1, 0], right[1, 0]], 0)
    high, low = halves(factors)
    return jnp.concatenate([high, high], 0), low


def diagonal_part(high, low, square):
    return dot(high, square[0], NT) + dot(high, square[1], NT) + dot(low, square[0], NT)


def coefficients(high, low, narrow):
    both = dot(high, narrow[0], NT)
    rank = both.shape[1] // 2
    return both[:, :rank] + both[:, rank:] + dot(low, narrow[1], NT)


def coupling_part(coefs, factors):
    high, low = halves(coefs)
    return dot(jnp.concatenate([high, low], 1), factors[0], NN) + dot(high, factors[1], NN)


def gathered(coef_ref, start, rows, stride, limit):
    here = coef_ref[pl.ds(start, rows)]
    lane = lax.broadcasted_iota(jnp.int32, here.shape, 1)
    quarter = here.shape[1] // 4
    ahead_x = coef_ref[pl.ds(pl.multiple_of(start + stride, 8), rows)]
    behind_x = coef_ref[pl.ds(pl.multiple_of(start - stride, 8), rows)]
    ahead_y = pltpu.roll(here, rows - 1, 0)
    behind_y = pltpu.roll(here, 1, 0)
    along_x = jnp.where(lane < quarter, ahead_x, behind_x)
    along_y = jnp.where(lane < 3 * quarter, ahead_y, behind_y)
    picked = jnp.where(lane < 2 * quarter, along_x, along_y)
    level = lax.rem(lane, quarter)
    return jnp.where(level < limit, picked, 0.0)


def operated(ref, start, rows, stride):
    here = ref[pl.ds(start, rows)]
    width = here.shape[1]
    beside = ref[pl.ds(pl.multiple_of(start + stride, 8), rows)]
    beside = beside + ref[pl.ds(pl.multiple_of(start - stride, 8), rows)]
    beside = beside + pltpu.roll(here, rows - 1, 0) + pltpu.roll(here, 1, 0)
    beside = beside + pltpu.roll(here, width - 1, 1) + pltpu.roll(here, 1, 1)
    return DIAGONAL * here - beside


def pack_kernel(source, block, low_x, high_x, low_y, high_y, arrived):
    cells_x, cells_y, _ = block.shape
    step = cells_x // arrived.shape[0]
    parts = [pl.ds(i * step, step) for i in range(arrived.shape[0])]
    copies = [pltpu.make_async_copy(source.at[p], block.at[p], arrived.at[i]) for i, p in enumerate(parts)]
    for copy in copies:
        copy.start()
    for copy, part in zip(copies, parts):
        copy.wait()
        for j in range(DEPTH):
            low_y[j, part] = block[part, j]
            high_y[j, part] = block[part, cells_y - DEPTH + j]
    low_x[...] = block[pl.ds(0, DEPTH)]
    high_x[...] = block[pl.ds(cells_x - DEPTH, DEPTH)]


def corner_kernel(low_y, high_y, low_x, high_x):
    near = DEPTH - 1
    cells_x = low_y.shape[1]
    for ref, first in ((low_x, 0), (high_x, cells_x - near)):
        at = pl.ds(first, near)
        ref[pl.ds(0, near)] = low_y[pl.ds(1, near), at]
        ref[pl.ds(near, near)] = high_y[pl.ds(0, near), at]


def table_kernel(stride, cells_x, cells_y, ranks, limit, rows, arrived):
    length_x, length_y = ranks.shape[2], ranks.shape[3]
    begin = lax.axis_index("gx") * cells_x
    parts = (
        (lax.rem(begin - PAD + length_x, length_x), 0, PAD),
        (begin, PAD, cells_x),
        (lax.rem(begin + cells_x, length_x), PAD + cells_x, PAD),
    )
    copies = [
        pltpu.make_async_copy(
            ranks.at[e, 0, pl.ds(pl.multiple_of(source, 8), size)],
            rows.at[e, pl.ds(target, size)],
            arrived.at[e, k],
        )
        for e in range(2)
        for k, (source, target, size) in enumerate(parts)
    ]
    for copy in copies:
        copy.start()
    for copy in copies:
        copy.wait()
    turn = lax.rem(PAD + length_y - lax.axis_index("gy") * cells_y, length_y)
    tall = rows.shape[1]
    here = [pltpu.roll(pltpu.roll(rows[e], turn, 1), tall - PAD + DEPTH, 0) for e in range(2)]
    kinds = (here[0], pltpu.roll(here[0], 1, 0), here[1], pltpu.roll(here[1], 1, 1))
    shape = (tall, limit.shape[1])
    kind = lax.broadcasted_iota(jnp.int32, shape, 1) // (shape[1] // 4)
    for y in range(PAD - DEPTH + 1, PAD + cells_y + DEPTH - 1):
        column = [jnp.broadcast_to(k[:, y : y + 1], shape) for k in kinds]
        along_x = jnp.where(kind == 0, column[0], column[1])
        along_y = jnp.where(kind == 2, column[2], column[3])
        limit[pl.ds(y, tall, stride=stride)] = jnp.where(kind < 2, along_x, along_y)


def own_kernel(stride, block, inverse, left, right, diag_out, coef_out):
    cells_x, cells_y, width = block.shape
    square, narrow = inward(inverse, left, right)
    step = largest_divisor(cells_x, 8)

    def body(i, carry):
        rows = block[pl.ds(i * step, step)].reshape(step * cells_y, width)
        high, low = halves(rows)
        diag = diagonal_part(high, low, square)
        coef = coefficients(high, low, narrow)
        for j in range(step):
            at = pl.multiple_of((i * step + j + DEPTH) * stride + PAD, 8)
            diag_out[pl.ds(at, cells_y)] = diag[j * cells_y : (j + 1) * cells_y]
            coef_out[pl.ds(at, cells_y)] = coef[j * cells_y : (j + 1) * cells_y]
        return carry

    lax.fori_loop(0, cells_x // step, body, 0, unroll=True)


def side_kernel(stride, diag_in, coef_in, low_x, high_x, low_y, high_y, inverse, left, right, diag_out, coef_out, turned):
    square, narrow = inward(inverse, left, right)
    depth, cells_y, width = low_x.shape
    cells_x = low_y.shape[1]
    for ref, first in ((low_x, 0), (high_x, DEPTH + cells_x)):
        high, low = halves(ref[...].reshape(depth * cells_y, width))
        diag = diagonal_part(high, low, square)
        coef = coefficients(high, low, narrow)
        for j in range(depth):
            at = (first + j) * stride + PAD
            diag_out[pl.ds(at, cells_y)] = diag[j * cells_y : (j + 1) * cells_y]
            coef_out[pl.ds(at, cells_y)] = coef[j * cells_y : (j + 1) * cells_y]
    for ref, inside, edge in ((low_y, PAD - DEPTH, 0), (high_y, 0, PAD + cells_y)):
        high, low = halves(ref[...].reshape(depth * cells_x, width))
        diag = diagonal_part(high, low, square)
        coef = coefficients(high, low, narrow)
        for j in range(depth):
            part = slice(j * cells_x, (j + 1) * cells_x)
            at = pl.ds(inside + j, cells_x, stride=PAD)
            for k in range(width // 128):
                turned[k, at] = diag[part, k * 128 : (k + 1) * 128]
            turned[width // 128, at] = coef[part]

        def place(x, carry):
            here = pl.ds(pl.multiple_of(x * PAD, 8), PAD)
            at = pl.ds(pl.multiple_of((x + DEPTH) * stride + edge, 8), PAD)
            for k in range(width // 128):
                diag_out[at, pl.ds(k * 128, 128)] = turned[k, here]
            coef_out[at] = turned[width // 128, here]
            return carry

        lax.fori_loop(0, cells_x, place, 0, unroll=4)


def chain_kernel(
    stride, diag_in, coef_in, low_x, high_x, limit, block, inverse, left, right,
    first, coef, first_image, second, sums,
):
    cells_x, cells_y, width = block.shape
    square, narrow = inward(inverse, left, right)
    factors = outward(left, right)
    near = DEPTH - 1

    for ref, edge, sign in ((low_x, DEPTH - near, -1), (high_x, DEPTH + cells_x, 1)):
        count = ref.shape[0] * ref.shape[1]
        high, low = halves(ref[...].reshape(count, width))
        diag = diagonal_part(high, low, square)
        coefs = coefficients(high, low, narrow)
        for j in range(2 * near):
            away_y = near - j if j < near else j - near + 1
            y = PAD - away_y if j < near else PAD + cells_y + away_y - 1
            for i in range(near):
                away_x = near - i if sign < 0 else i + 1
                if away_x + away_y <= DEPTH:
                    at = (edge + i) * stride + y
                    row = j * near + i
                    first[pl.ds(at, 1)] = diag[row : row + 1]
                    coef[pl.ds(at, 1)] = coefs[row : row + 1]

    def slabs(begin, end, most):
        step = largest_divisor(end - begin, most)
        return [(x, step) for x in range(begin, end, step)]

    def inside(value, x, step):
        value = value.reshape(step, stride, value.shape[1])[:, PAD : PAD + cells_y]
        return value[max(DEPTH - x, 0) : max(DEPTH + cells_x - x, 0)]

    def owned(x, step):
        return max(x - DEPTH, 0), min(x + step - DEPTH, cells_x)

    def summed(value):
        return jnp.sum(value.reshape(-1, 8, width), 0)

    totals = [jnp.zeros((8, width), F32)] * 6
    last = 2 * DEPTH + cells_x
    for x, step in slabs(1, last - 1, 9):
        at = pl.ds(x * stride, step * stride)
        picked = gathered(coef, x * stride, step * stride, stride, limit[at])
        first[at] = first[at] + coupling_part(picked, factors)
    for x, step in slabs(2, last - 2, 9):
        at = pl.ds(x * stride, step * stride)
        image = operated(first, x * stride, step * stride, stride)
        first_image[at] = image
        high, low = halves(image)
        second[at] = diagonal_part(high, low, square)
        coef[at] = coefficients(high, low, narrow)
        begin, end = owned(x, step)
        if begin < end:
            field = inside(first[at], x, step)
            totals[0] += summed(block[pl.ds(begin, end - begin)] * field)
            totals[1] += summed(inside(image, x, step) * field)
    for x, step in slabs(3, last - 3, 9):
        at = pl.ds(x * stride, step * stride)
        picked = gathered(coef, x * stride, step * stride, stride, limit[at])
        field = second[at] + coupling_part(picked, factors)
        second[at] = field
        begin, end = owned(x, step)
        if begin < end:
            field = inside(field, x, step)
            totals[2] += summed(block[pl.ds(begin, end - begin)] * field)
            totals[3] += summed(inside(first_image[at], x, step) * field)
            totals[4] += summed(field * field)
    for x, step in slabs(DEPTH, DEPTH + cells_x, 8):
        start, rows = x * stride, step * stride
        here = second[pl.ds(start, rows)]
        beside = second[pl.ds(start + stride, rows)] + pltpu.roll(here, rows - 1, 0) + pltpu.roll(here, width - 1, 1)
        totals[5] += summed(inside(here * beside, x, step))
    totals = totals[:4] + [DIAGONAL * totals[4] - 2.0 * totals[5]]
    rows = [jnp.sum(jnp.sum(p, 0, keepdims=True), 1, keepdims=True) for p in totals]
    for i, row in enumerate(rows):
        sums[pl.ds(i, 1)] = jnp.broadcast_to(row, (1, sums.shape[1]))
    sums[pl.ds(5, 3)] = jnp.zeros((3, sums.shape[1]), F32)


def last_kernel(stride, begin, field, limit, inverse, left, right, image_out, out, image, coef):
    step, cells_y, width = out.shape
    square, narrow = inward(inverse, left, right)
    factors = outward(left, right)
    start = (begin + DEPTH) * stride
    part = largest_divisor(step + 2, 9)
    for x in range(0, step + 2, part):
        at = pl.ds(x * stride, part * stride)
        value = operated(field, start + (x - 1) * stride, part * stride, stride)
        image[at] = value
        coef[at] = coefficients(*halves(value), narrow)
    picked = gathered(coef, stride, step * stride, stride, limit[pl.ds(start, step * stride)])
    picked = picked.reshape(step, stride, picked.shape[1])[:, PAD : PAD + cells_y]
    rows = image[pl.ds(stride, step * stride)].reshape(step, stride, width)[:, PAD : PAD + cells_y]
    image_out[...] = rows
    high, low = halves(rows.reshape(step * cells_y, width))
    total = diagonal_part(high, low, square)
    total = total + coupling_part(picked.reshape(step * cells_y, picked.shape[2]), factors)
    out[...] = total.reshape(step, cells_y, width)


def combine_kernel(stride, step, pieces, sums, block, z_ref, w_ref, u_ref, *rest):
    v_refs, y_refs, rest = rest[0 : 2 * pieces : 2], rest[1 : 2 * pieces : 2], rest[2 * pieces :]
    outs, buffers, sent = rest[:3], rest[3:6], rest[6]
    cells_x, cells_y, width = block.shape
    rz, zw, ru, wu, uv = (sums[pl.ds(k, 1), pl.ds(0, 128)] for k in range(5))
    alpha = rz / zw
    rz_next = alpha * (alpha * wu - ru)
    ratio = rz_next / rz
    grown = 1.0 + ratio
    curve = grown * (grown * zw - 2.0 * alpha * wu) + alpha * alpha * uv
    alpha_next = rz_next / curve
    s = jnp.concatenate([alpha + alpha_next * grown] * (width // 128), 1)
    t = jnp.concatenate([alpha * alpha_next] * (width // 128), 1)

    def copies(chunk):
        part = pl.ds(chunk * step, step)
        return [
            pltpu.make_async_copy(buffer.at[part], out.at[part], sent.at[k, chunk])
            for k, (buffer, out) in enumerate(zip(buffers, outs))
        ]

    per = cells_x // pieces // step

    def work(i, carry, k):
        chunk = k * per + i
        for j in range(step):
            x = chunk * step + j
            at = pl.ds(pl.multiple_of((x + DEPTH) * stride + PAD, 8), cells_y)
            z0, w0, u0 = z_ref[at], w_ref[at], u_ref[at]
            buffers[0][x] = s * z0 - t * u0
            buffers[1][x] = (block[x] - s * w0) + t * v_refs[k][i * step + j]
            buffers[2][x] = (z0 - s * u0) + t * y_refs[k][i * step + j]
        for copy in copies(chunk):
            copy.start()
        return carry

    for k in range(pieces):
        lax.fori_loop(0, per, lambda i, carry, k=k: work(i, carry, k), 0, unroll=True)

    def finish(chunk, carry):
        for copy in copies(chunk):
            copy.wait()
        return carry

    lax.fori_loop(0, cells_x // step, finish, 0)


def resident(*values):
    return tuple(pltpu.with_memory_space_constraint(v, pltpu.VMEM) for v in values)


def neighbour(value, axis, offset):
    count = lax.axis_size(axis)
    return lax.ppermute(value, axis, [(i, (i + offset) % count) for i in range(count)])


def total_over(value, axis):
    count = lax.axis_size(axis)
    if count & (count - 1):
        return lax.psum(value, axis)
    groups, hop = [], 1
    if count.bit_length() % 2 == 0:
        groups, hop = [(1,)], 2
    while hop < count:
        groups.append((2 * hop, hop, 3 * hop))
        hop *= 4
    for hops in groups:
        moved = [lax.ppermute(value, axis, [(i, i ^ h) for i in range(count)]) for h in hops]
        value = sum(moved, value)
    return value


def call(kernel, out_shape, inputs, specs=None, **kwargs):
    return pl.pallas_call(
        kernel, out_shape=out_shape, in_specs=specs or [WHOLE] * len(inputs), compiler_params=GRANT, **kwargs
    )(*inputs)


def per_device(right_side, block_inverse, basis_left, basis_right, ranks):
    cells_x, cells_y, width = right_side.shape
    stride = cells_y + 2 * PAD
    lines = (cells_x + 2 * DEPTH) * stride
    tall = cells_x + 2 * PAD
    rank4 = 4 * basis_left.shape[2]
    near = DEPTH - 1
    weights = resident(block_inverse, basis_left, basis_right)
    wide = pltpu.VMEM((lines, width), F32)
    slim = pltpu.VMEM((lines, rank4), F32)
    edge_x = pltpu.VMEM((DEPTH, cells_y, width), F32)
    edge_y = pltpu.VMEM((DEPTH, cells_x, width), F32)
    corner = pltpu.VMEM((2 * near, near, width), F32)

    anywhere = pl.BlockSpec(memory_space=pltpu.HBM)
    block, out_x, in_x, out_y, in_y = call(
        pack_kernel, (pltpu.VMEM(right_side.shape, F32), edge_x, edge_x, edge_y, edge_y), (pltpu.with_memory_space_constraint(right_side, pltpu.HBM),),
        [anywhere], out_specs=(WHOLE,) * 5,
        scratch_shapes=[pltpu.SemaphoreType.DMA((cells_x // largest_divisor(cells_x, 8),))],
    )
    (block,) = resident(block)
    low_y = neighbour(in_y, "gy", 1)
    high_y = neighbour(out_y, "gy", -1)
    low_x = neighbour(in_x, "gx", 1)
    high_x = neighbour(out_x, "gx", -1)

    diag, coef = call(lambda *refs: own_kernel(stride, *refs), (wide, slim), (block, *weights), out_specs=(WHOLE,) * 2)
    limit = call(
        lambda *refs: table_kernel(stride, cells_x, cells_y, *refs),
        pltpu.VMEM((tall * stride, rank4), jnp.int32), (ranks,), [pl.BlockSpec(memory_space=pl.ANY)],
        out_specs=WHOLE,
        scratch_shapes=[pltpu.VMEM((2, tall, ranks.shape[3]), jnp.int32), pltpu.SemaphoreType.DMA((2, 3))],
    )

    corners = call(corner_kernel, (corner, corner), resident(low_y, high_y), out_specs=(WHOLE,) * 2)
    corner_low = neighbour(corners[1], "gx", 1)
    corner_high = neighbour(corners[0], "gx", -1)

    diag, coef = call(
        lambda *refs: side_kernel(stride, *refs), (wide, slim),
        (*resident(diag, coef, low_x, high_x, low_y, high_y), *weights), out_specs=(WHOLE,) * 2,
        input_output_aliases={0: 0, 1: 1},
        scratch_shapes=[pltpu.VMEM((width // 128 + 1, cells_x * PAD, 128), F32)],
    )

    first, _, first_image, second, sums = call(
        lambda *refs: chain_kernel(stride, *refs),
        (wide, slim, wide, wide, pltpu.VMEM((8, 128), F32)),
        (*resident(diag, coef, corner_low, corner_high, limit), block, *weights), out_specs=(WHOLE,) * 5,
        input_output_aliases={0: 0, 1: 1},
    )

    sums = total_over(total_over(sums, "gx"), "gy")

    pieces = 4 if cells_x % 4 == 0 else 1
    step = cells_x // pieces
    piece = pltpu.VMEM((step, cells_y, width), F32)
    last = [
        array
        for k in range(pieces)
        for array in call(
            lambda *refs, k=k: last_kernel(stride, k * step, *refs), (piece, piece),
            (*resident(second, limit), *weights), out_specs=(WHOLE,) * 2,
            scratch_shapes=[pltpu.VMEM(((step + 2) * stride, n), F32) for n in (width, rank4)],
        )
    ]

    chunk = largest_divisor(step, 8)
    out = jax.ShapeDtypeStruct((cells_x, cells_y, width), F32)
    return call(
        lambda *refs: combine_kernel(stride, chunk, pieces, *refs), (out,) * 3,
        (*resident(sums), block, *resident(first, first_image, second, *last)),
        out_specs=(anywhere,) * 3,
        scratch_shapes=[pltpu.VMEM((cells_x, cells_y, width), F32)] * 3
        + [pltpu.SemaphoreType.DMA((3, cells_x // chunk))],
    )


def solution(mesh):
    placed = (P("gx", "gy", None), P(), P(), P(), P())

    return jax.shard_map(
        per_device,
        mesh=mesh,
        in_specs=placed,
        out_specs=(P("gx", "gy", None), P("gx", "gy", None), P("gx", "gy", None)),
        check_vma=False,
    )
```
